128 devices in a mesh: kv: 2 (over z_lo), batch: 64 (over z_hi, x, y, core).
Axes of the slice: x: 4, y: 4, z: 4 (z_hi: 2, z_lo: 2; z = z_hi * 2 + z_lo), core: 2. Of those that a mesh axis runs over, the one named last changes fastest.
Arguments:
- queries: bfloat16 [256, 32, 128], P(('kv', 'batch')), may hold values from -64 to 64
- prefix_keys: bfloat16 [8192, 8, 128], P('batch', 'kv'), may hold values from -6 to 6
- prefix_values: bfloat16 [8192, 8, 128], P('batch', 'kv'), may hold values from -6 to 6
- suffix_keys: bfloat16 [256, 2048, 8, 128], P('batch', None, 'kv'), may hold values from -6 to 6
- suffix_values: bfloat16 [256, 2048, 8, 128], P('batch', None, 'kv'), may hold values from -6 to 6
- suffix_lengths: int32 [256], P('batch'), may hold values from 512 to 2048, as said below
- slot_sequence: int32 [256], P('batch'), may hold values from 0 to 255, as said below
Outputs:
- attended: bfloat16 [256, 32, 128], P(('kv', 'batch'))
The draws below stay inside these ranges and needn't reach their ends.
Inputs may be any that keep to these rules, and one draw needn't show every extreme that they name: `suffix_lengths`: some slot holds exactly 2048 live tokens. `slot_sequence`: each sequence's suffix occupies exactly one slot; the 256 / 64 slots of one index of batch hold sequences whose output rows lie on pairwise different indices of batch.
All inputs are finite; a program needn't handle non-finite values.
Results may differ from the reference program's by a relative error of at most 0.007.
Values may be sent and summed in bfloat16 or wider, within the bound.
No kernel may reach another device: no remote copies, remote signals or barrier semaphores. Data moves between devices by JAX's collectives and lax.ppermute only.
A program may use at most 64 MiB of HBM per device.

```python
import jax
import jax.numpy as jnp
from jax import lax

HEADS = 32
KV_HEADS = 8
HEAD_DIM = 128
SEQ_DEV = 2
PREFIX = 8192
SUFFIX = 2048
BATCH = 256
N_BATCH = 64


def draw_queries(key, part):
    sampled = jnp.clip(2.5 * jax.random.normal(jax.random.fold_in(key, 1), (BATCH, HEADS, HEAD_DIM), jnp.float32), -15.0, 15.0)
    return sampled.astype(jnp.bfloat16)


def draw_prefix_keys(key, part):
    sampled = jnp.clip(jax.random.normal(jax.random.fold_in(key, 2), (PREFIX, KV_HEADS, HEAD_DIM), jnp.float32), -6.0, 6.0)
    return sampled.astype(jnp.bfloat16)


def draw_suffix_keys(key, part):
    sampled = jnp.clip(jax.random.normal(jax.random.fold_in(key, 3), (BATCH, SUFFIX, KV_HEADS, HEAD_DIM), jnp.float32), -6.0, 6.0)
    return sampled.astype(jnp.bfloat16)


def draw_suffix_lengths(key, part):
    drawn = jax.random.randint(jax.random.fold_in(key, 4), (BATCH,), SUFFIX // 4, SUFFIX + 1, jnp.int32)
    longest = jax.random.randint(jax.random.fold_in(key, 5), (), 0, BATCH, jnp.int32)
    return jnp.where(jnp.arange(BATCH) == longest, SUFFIX, drawn).astype(jnp.int32)


def draw_slot_sequence(key, part):
    per_index = BATCH // N_BATCH
    offsets = jax.random.permutation(jax.random.fold_in(key, 21), N_BATCH).astype(jnp.int32)
    shifts = jax.random.permutation(jax.random.fold_in(key, 22), N_BATCH)[:per_index].astype(jnp.int32)
    column = (offsets[:, None] + shifts[None, :]) % N_BATCH
    member_key = jax.random.fold_in(key, 23)
    member_table = jax.vmap(lambda index: jax.random.permutation(jax.random.fold_in(member_key, index), per_index))(jnp.arange(N_BATCH)).astype(jnp.int32)
    ranks = jnp.arange(per_index).astype(jnp.int32)
    member = member_table[column, ranks[None, :]]
    group = member // SEQ_DEV
    within = member % SEQ_DEV
    sequence = (group * N_BATCH + column) * SEQ_DEV + within
    return sequence.reshape(BATCH).astype(jnp.int32)


def level_of(stream_key, shape, cuts, smallest, top_value):
    loudness, own = 1.0, jax.random.fold_in(stream_key, 6)
    for axis_at, blocks in cuts:
        steps = jnp.exp(jax.random.uniform(jax.random.fold_in(own, axis_at), (blocks,), jnp.float32, smallest / len(cuts), top_value / len(cuts)))
        loudness = loudness * jnp.repeat(steps, shape[axis_at] // blocks).reshape([-1 if axis == axis_at else 1 for axis in range(len(shape))])
    return loudness


def centred(rng, dims, spread, reach, cuts=(), dtype=jnp.bfloat16):
    values = spread * jax.random.normal(rng, dims, jnp.float32)
    if cuts:
        values = values * level_of(rng, dims, cuts, -0.22, 0.18)
    return jnp.clip(values, -reach, reach).astype(dtype)


def setup_inputs(seed: int = 0) -> dict:
    arg_keys = jax.random.split(jax.random.key(seed), 8)
    queries = draw_queries(jax.random.fold_in(arg_keys[7], 71), 0)
    prefix_keys = draw_prefix_keys(jax.random.fold_in(arg_keys[7], 71), 0)
    prefix_values = centred(arg_keys[2], (PREFIX, KV_HEADS, HEAD_DIM), 1.0, 6.0, ((0, 64), (1, 2)))
    suffix_keys = draw_suffix_keys(jax.random.fold_in(arg_keys[7], 71), 0)
    suffix_values = centred(arg_keys[4], (BATCH, SUFFIX, KV_HEADS, HEAD_DIM), 1.0, 6.0, ((0, 64), (2, 2)))
    suffix_lengths = draw_suffix_lengths(jax.random.fold_in(arg_keys[7], 71), 0)
    slot_sequence = draw_slot_sequence(jax.random.fold_in(arg_keys[7], 71), 0)
    return {"queries": queries, "prefix_keys": prefix_keys, "prefix_values": prefix_values, "suffix_keys": suffix_keys, "suffix_values": suffix_values, "suffix_lengths": suffix_lengths, "slot_sequence": slot_sequence}


negative_fill = -1e30


def reference(queries, prefix_keys, prefix_values, suffix_keys, suffix_values, suffix_lengths, slot_sequence):
    group_size = HEADS // KV_HEADS
    scale = HEAD_DIM ** -0.5
    grouped = queries.reshape(BATCH, KV_HEADS, group_size, HEAD_DIM).transpose(1, 0, 2, 3)

    def prefix_head(operands):
        query_head, key_head, value_head = operands
        scores = jnp.einsum("bjd,td->bjt", query_head.astype(jnp.float32), key_head.astype(jnp.float32)) * scale
        best = jnp.max(scores, axis=-1)
        weights = jnp.exp(scores - best[..., None])
        total = jnp.sum(weights, axis=-1)
        rounded = lax.optimization_barrier(weights.astype(jnp.bfloat16))
        accum = jnp.einsum("bjt,td->bjd", rounded.astype(jnp.float32), value_head.astype(jnp.float32))
        return best, total, accum

    pre_best, pre_total, pre_acc = lax.map(prefix_head, (grouped, prefix_keys.transpose(1, 0, 2), prefix_values.transpose(1, 0, 2)))
    pre_best = pre_best.transpose(1, 0, 2).reshape(BATCH, HEADS)
    pre_total = pre_total.transpose(1, 0, 2).reshape(BATCH, HEADS)
    pre_acc = pre_acc.transpose(1, 0, 2, 3).reshape(BATCH, HEADS, HEAD_DIM)

    slot_queries = queries[slot_sequence].reshape(BATCH, KV_HEADS, group_size, HEAD_DIM)
    position = jnp.arange(SUFFIX).astype(jnp.int32)

    def suffix_slot(operands):
        query_slot, key_slot, value_slot, length = operands
        scores = jnp.einsum("kjd,tkd->kjt", query_slot.astype(jnp.float32), key_slot.astype(jnp.float32)) * scale
        scores = jnp.where(position[None, None, :] < length, scores, negative_fill)
        best = jnp.max(scores, axis=-1)
        weights = jnp.exp(scores - best[..., None])
        total = jnp.sum(weights, axis=-1)
        rounded = lax.optimization_barrier(weights.astype(jnp.bfloat16))
        accum = jnp.einsum("kjt,tkd->kjd", rounded.astype(jnp.float32), value_slot.astype(jnp.float32))
        return best, total, accum

    suf_best, suf_total, suf_acc = lax.map(suffix_slot, (slot_queries, suffix_keys, suffix_values, suffix_lengths))
    seq_best = jnp.zeros((BATCH, HEADS), jnp.float32).at[slot_sequence].set(suf_best.reshape(BATCH, HEADS))
    seq_total = jnp.zeros((BATCH, HEADS), jnp.float32).at[slot_sequence].set(suf_total.reshape(BATCH, HEADS))
    seq_acc = jnp.zeros((BATCH, HEADS, HEAD_DIM), jnp.float32).at[slot_sequence].set(suf_acc.reshape(BATCH, HEADS, HEAD_DIM))
    top = jnp.maximum(pre_best, seq_best)
    first = jnp.exp(pre_best - top)
    second = jnp.exp(seq_best - top)
    numerator = pre_acc * first[..., None] + seq_acc * second[..., None]
    denominator = pre_total * first + seq_total * second
    return (numerator / denominator[..., None]).astype(jnp.bfloat16)
```

```python
import jax
import jax.numpy as jnp
from jax import lax
from jax.experimental import pallas as pl
from jax.experimental.pallas import tpu as pltpu
from jax.sharding import Mesh
from jax.sharding import PartitionSpec as P

negative_fill = -1e30
f32 = jnp.float32
bf16 = jnp.bfloat16
vmem = pl.BlockSpec(memory_space=pltpu.VMEM)
smem = pl.BlockSpec(memory_space=pltpu.SMEM)


def limit(mib):
    return pltpu.CompilerParams(vmem_limit_bytes=mib << 20)


def rounded(x):
    return x.astype(bf16).astype(f32)


def nt_dot(a, b):
    return lax.dot_general(a, b, (((1,), (1,)), ((), ())), preferred_element_type=f32)


def ask_kernel(queries_ref, out_ref):
    groups, copies = out_ref.shape[:2]
    sub8 = lax.broadcasted_iota(jnp.int32, (8, out_ref.shape[3]), 0)
    for g in range(groups):
        tiles = []
        for k in (0, 2):
            base = 16 * g + 4 * k
            one = queries_ref[0, base : base + 8, :].astype(f32)
            two = queries_ref[1, base : base + 8, :].astype(f32)
            tiles.append(jnp.where(sub8 < 4, one, pltpu.roll(two, 4, 0)))
            tiles.append(jnp.where(sub8 < 4, pltpu.roll(one, 4, 0), two))
        piece = jnp.concatenate(tiles, axis=0).astype(bf16)
        for c in range(copies):
            out_ref[g, c] = piece


def prefix_kernel(q_ref, k0_ref, k1_ref, v0_ref, v1_ref, out_ref):
    pieces = q_ref.shape[0]
    kv_local, _, dim = k0_ref.shape
    scale = dim ** (-0.5)
    rows = pieces * 8
    lane = lax.broadcasted_iota(jnp.int32, (rows, 128), 1)
    stat = jnp.zeros((rows, 128), f32)
    for k in range(kv_local):
        q = q_ref[:, 8 * k : 8 * k + 8, :].astype(f32).reshape(rows, dim).astype(bf16)
        keys = jnp.concatenate([k0_ref[k], k1_ref[k]], axis=0)
        values = jnp.concatenate([v0_ref[k], v1_ref[k]], axis=0)
        scores = nt_dot(q, keys) * scale
        best = rounded(jnp.max(scores, axis=1, keepdims=True))
        weights = jnp.exp(scores - best)
        total = jnp.sum(weights, axis=1, keepdims=True)
        acc = jnp.dot(weights.astype(bf16), values, preferred_element_type=f32)
        out_ref[:, 8 * k : 8 * k + 8, :] = acc.reshape(pieces, 8, dim).astype(bf16)
        high = rounded(total)
        stat = jnp.where(lane == 4 * k, best, stat)
        stat = jnp.where(lane == 4 * k + 1, high, stat)
        stat = jnp.where(lane == 4 * k + 2, total - high, stat)
    out_ref[:, 8 * kv_local : 8 * kv_local + 8, :] = stat.reshape(pieces, 8, 128).astype(bf16)


def place_of(sequence, batch_count, per_device):
    device = sequence // per_device
    return device // 2, device % 2, sequence % per_device


def suffix_kernel(ids_ref, len_ref, mine_ref, other_ref, keys_ref, values_ref, out_ref):
    slots, wide, dim = keys_ref.shape
    scale = dim ** (-0.5)
    chunk = 1024
    row = lax.broadcasted_iota(jnp.int32, (16, chunk), 0)
    lane = lax.broadcasted_iota(jnp.int32, (16, chunk), 1)
    own_head = lane % 4 == row // 4
    position = lane // 4
    sub8 = lax.broadcasted_iota(jnp.int32, (8, dim), 0)
    lane8 = lax.broadcasted_iota(jnp.int32, (8, dim), 1)
    for s in range(slots):
        piece, core, i = place_of(ids_ref[s], 0, 2)
        length = len_ref[s]
        here = core == lax.axis_index("core")
        q = jnp.where(here, mine_ref[piece].astype(f32), other_ref[piece].astype(f32))
        pairs = []
        for k in (0, 2):
            even, odd = q[8 * k : 8 * k + 8], q[8 * k + 8 : 8 * k + 16]
            even = jnp.where(i == 0, even, pltpu.roll(even, 4, 0))
            odd = jnp.where(i == 0, pltpu.roll(odd, 4, 0), odd)
            pairs.append(jnp.where(sub8 < 4, even, odd))
        q16 = jnp.concatenate(pairs, axis=0).astype(bf16)
        parts = []
        peak = jnp.full((16, 128), negative_fill, f32)
        for c in range(wide // chunk):
            part = nt_dot(q16, keys_ref[s, c * chunk : (c + 1) * chunk, :]) * scale
            keep = own_head & (position < length - c * (chunk // 4))
            part = jnp.where(keep, part, negative_fill)
            for t in range(chunk // 128):
                peak = jnp.maximum(peak, part[:, 128 * t : 128 * t + 128])
            parts.append(part)
        best = rounded(jnp.max(peak, axis=1, keepdims=True))
        sums = jnp.zeros((16, 128), f32)
        acc = jnp.zeros((16, dim), f32)
        for c in range(wide // chunk):
            weights = jnp.exp(parts[c] - best)
            for t in range(chunk // 128):
                sums = sums + weights[:, 128 * t : 128 * t + 128]
            acc = acc + jnp.dot(
                weights.astype(bf16),
                values_ref[s, c * chunk : (c + 1) * chunk, :],
                preferred_element_type=f32,
            )
        total = jnp.sum(sums, axis=1, keepdims=True)
        best, total = jnp.broadcast_to(best, (16, dim)), jnp.broadcast_to(total, (16, dim))
        stat = jnp.zeros((8, dim), f32)
        for k in range(4):
            half = slice(8 * (k // 2), 8 * (k // 2) + 8)

            def spread(x):
                x = x[half]
                return jnp.where(i == k % 2, x, pltpu.roll(x, 4, 0))

            out_ref[s, 8 * k : 8 * k + 8, :] = spread(acc)
            stat = jnp.where(lane8 == 4 * k, spread(best), stat)
            stat = jnp.where(lane8 == 4 * k + 1, spread(total), stat)
        out_ref[s, 32:40, :] = stat


def merge_kernel(ids_ref, ids_other_ref, part_ref, mine_ref, other_ref, out_ref):
    del part_ref
    sub8 = lax.broadcasted_iota(jnp.int32, (8, 128), 0)
    lane8 = lax.broadcasted_iota(jnp.int32, (8, 128), 1)

    def one(ids, results, s):
        piece, core, i = place_of(ids[s], 0, 2)

        @pl.when(core == lax.axis_index("core"))
        def _():
            used = sub8 // 4 == i
            old = out_ref[piece, 32:40, :].astype(f32)
            new = results[s, 32:40, :]
            stat = old
            for k in range(4):
                best_old, high, low = (old[:, 4 * k + c : 4 * k + c + 1] for c in range(3))
                best_new, total_new = (new[:, 4 * k + c : 4 * k + c + 1] for c in range(2))
                best = jnp.maximum(best_old, best_new)
                first = jnp.broadcast_to(jnp.exp(best_old - best), (8, 128))
                second = jnp.broadcast_to(jnp.exp(best_new - best), (8, 128))
                total = (high + low) * first + total_new * second
                acc_old = out_ref[piece, 8 * k : 8 * k + 8, :].astype(f32)
                acc = acc_old * first + results[s, 8 * k : 8 * k + 8, :] * second
                out_ref[piece, 8 * k : 8 * k + 8, :] = jnp.where(used, acc, acc_old).astype(bf16)
                rest = rounded(total)
                stat = jnp.where(used & (lane8 == 4 * k), best, stat)
                stat = jnp.where(used & (lane8 == 4 * k + 1), rest, stat)
                stat = jnp.where(used & (lane8 == 4 * k + 2), total - rest, stat)
            out_ref[piece, 32:40, :] = stat.astype(bf16)

    for s in range(mine_ref.shape[0]):
        one(ids_ref, mine_ref, s)
        one(ids_other_ref, other_ref, s)


def combine_kernel(got_ref, out_ref):
    count = got_ref.shape[0] // 2
    sub8 = lax.broadcasted_iota(jnp.int32, (8, 128), 0)
    for half in range(2):
        at = slice(half * count, (half + 1) * count)
        stat = got_ref[at, 32:40, :].astype(f32)
        top = jnp.max(stat, axis=0, keepdims=True)
        factor = jnp.exp(stat - top)
        total = pltpu.roll(stat, 127, 2) + pltpu.roll(stat, 126, 2)
        factor = factor / jnp.sum(factor * total, axis=0, keepdims=True)
        rows = []
        for k in range(4):
            acc = got_ref[at, 8 * k : 8 * k + 8, :].astype(f32)
            rows.append(jnp.sum(acc * factor[:, :, 4 * k : 4 * k + 1], axis=0))
        for k in (0, 2):
            base = 16 * half + 4 * k
            turned = pltpu.roll(rows[k + 1], 4, 0)
            out_ref[0, base : base + 8, :] = jnp.where(sub8 < 4, rows[k], turned).astype(bf16)
            turned = pltpu.roll(rows[k], 4, 0)
            out_ref[1, base : base + 8, :] = jnp.where(sub8 < 4, turned, rows[k + 1]).astype(bf16)


def shards(
    queries, prefix_keys, prefix_values, suffix_keys, suffix_values, suffix_lengths, slot_sequence
):
    kv_count = lax.axis_size("kv")
    m_count = lax.axis_size("m")
    per_device, head_count, dim = queries.shape
    local_heads = head_count // kv_count
    kv_local = prefix_keys.shape[1]
    group = local_heads // kv_local
    pieces = kv_count * m_count
    slots, suffix_len = suffix_keys.shape[:2]
    swap = [(0, 1), (1, 0)]

    def across(x):
        return lax.ppermute(x, "core", swap)

    def exchange(x):
        return lax.all_to_all(x, ("kv", "m"), split_axis=0, concat_axis=0, tiled=True)

    sent = pl.pallas_call(
        ask_kernel,
        in_specs=[vmem],
        out_specs=vmem,
        out_shape=jax.ShapeDtypeStruct((kv_count, m_count, per_device * local_heads, dim), bf16),
        cost_estimate=pl.CostEstimate(flops=10**11, transcendentals=0, bytes_accessed=2**28),
        compiler_params=limit(4),
        name="ask",
    )(queries)
    mine = exchange(sent.reshape(pieces, per_device * local_heads, dim))

    keys = suffix_keys.reshape(slots, suffix_len * kv_local, dim)
    values = suffix_values.reshape(slots, suffix_len * kv_local, dim)
    keys_here, values_here = prefix_keys.transpose(1, 0, 2), prefix_values.transpose(1, 0, 2)
    keys_there, values_there = across(keys_here), across(values_here)
    ids_there = across(slot_sequence)

    other = across(mine)
    part = pl.pallas_call(
        prefix_kernel,
        in_specs=[vmem] * 5,
        out_specs=vmem,
        out_shape=jax.ShapeDtypeStruct((pieces, per_device * local_heads + 8, dim), bf16),
        cost_estimate=pl.CostEstimate(flops=10**9, transcendentals=0, bytes_accessed=2**21),
        compiler_params=limit(4),
        name="prefix",
    )(mine, keys_here, keys_there, values_here, values_there)

    found = pl.pallas_call(
        suffix_kernel,
        in_specs=[smem] * 2 + [vmem] * 4,
        out_specs=vmem,
        out_shape=jax.ShapeDtypeStruct((slots, per_device * local_heads + 8, dim), f32),
        cost_estimate=pl.CostEstimate(flops=10**9, transcendentals=0, bytes_accessed=2**21),
        compiler_params=limit(4),
        name="suffix",
    )(slot_sequence, suffix_lengths, mine, other, keys, values)
    found_there = across(found)

    part = pl.pallas_call(
        merge_kernel,
        in_specs=[smem] * 2 + [vmem] * 3,
        out_specs=vmem,
        out_shape=jax.ShapeDtypeStruct(part.shape, bf16),
        input_output_aliases={2: 0},
        compiler_params=limit(4),
        name="merge",
    )(slot_sequence, ids_there, part, found, found_there)

    got = exchange(part)
    return pl.pallas_call(
        combine_kernel,
        in_specs=[vmem],
        out_specs=vmem,
        out_shape=jax.ShapeDtypeStruct(queries.shape, bf16),
        compiler_params=limit(4),
        name="combine",
    )(got)


def solution(mesh):
    kv, batch = (mesh.shape[a] for a in ("kv", "batch"))
    fine = Mesh(mesh.devices.reshape(kv, batch // 2, 2), ("kv", "m", "core"))
    rows, positions = ("kv", "m", "core"), ("m", "core")
    return jax.shard_map(
        shards,
        mesh=fine,
        in_specs=(
            P(rows, None, None),
            P(positions, "kv", None),
            P(positions, "kv", None),
            P(positions, None, "kv", None),
            P(positions, None, "kv", None),
            P(positions),
            P(positions),
        ),
        out_specs=P(rows, None, None),
        check_vma=False,
    )
```

```python
import jax
import jax.numpy as jnp
from jax import lax
from jax.experimental import pallas as pl
from jax.experimental.pallas import tpu as pltpu
from jax.sharding import Mesh
from jax.sharding import PartitionSpec as P

negative_fill = -1e30
f32 = jnp.float32
bf16 = jnp.bfloat16
in_hbm = pl.BlockSpec(memory_space=pltpu.HBM)
vmem = pl.BlockSpec(memory_space=pltpu.VMEM)


def limit(mib):
    return pltpu.CompilerParams(vmem_limit_bytes=mib << 20)


def rounded(x):
    return x.astype(bf16).astype(f32)


def nt_dot(a, b):
    return lax.dot_general(a, b, (((1,), (1,)), ((), ())), preferred_element_type=f32)


def ask_kernel(queries_ref, out_ref):
    groups, copies = out_ref.shape[:2]
    sub8 = lax.broadcasted_iota(jnp.int32, (8, out_ref.shape[3]), 0)
    for g in range(groups):
        tiles = []
        for k in (0, 2):
            base = 16 * g + 4 * k
            one = queries_ref[0, base : base + 8, :].astype(f32)
            two = queries_ref[1, base : base + 8, :].astype(f32)
            tiles.append(jnp.where(sub8 < 4, one, pltpu.roll(two, 4, 0)))
            tiles.append(jnp.where(sub8 < 4, pltpu.roll(one, 4, 0), two))
        piece = jnp.concatenate(tiles, axis=0).astype(bf16)
        for c in range(copies):
            out_ref[g, c] = piece


def prefix_kernel(q_ref, k0_ref, v0_ref, k1_ref, v1_ref, out_ref, wide_ref):
    pieces = q_ref.shape[0]
    positions, kv_local, dim = k0_ref.shape
    scale = dim ** (-0.5)
    rows = pieces * 8
    lane = lax.broadcasted_iota(jnp.int32, (rows, 128), 1)
    stat = jnp.zeros((rows, 128), f32)
    for n, pair in enumerate(((k0_ref, k1_ref), (v0_ref, v1_ref))):
        for c, ref in enumerate(pair):
            wide_ref[n, c] = ref[...].astype(f32).reshape(positions * kv_local, dim)

    def block(n, k):
        parts = [wide_ref[n, c, pl.ds(k, positions, stride=kv_local), :] for c in range(2)]
        return jnp.concatenate(parts, axis=0).astype(bf16)

    for k in range(kv_local):
        q = q_ref[:, 8 * k : 8 * k + 8, :].astype(f32).reshape(rows, dim).astype(bf16)
        keys, values = block(0, k), block(1, k)
        scores = nt_dot(q, keys) * scale
        best = rounded(jnp.max(scores, axis=1, keepdims=True))
        weights = jnp.exp(scores - best)
        total = jnp.sum(weights, axis=1, keepdims=True)
        acc = jnp.dot(weights.astype(bf16), values, preferred_element_type=f32)
        out_ref[:, 8 * k : 8 * k + 8, :] = acc.reshape(pieces, 8, dim).astype(bf16)
        high = rounded(total)
        stat = jnp.where(lane == 4 * k, best, stat)
        stat = jnp.where(lane == 4 * k + 1, high, stat)
        stat = jnp.where(lane == 4 * k + 2, total - high, stat)
    out_ref[:, 8 * kv_local : 8 * kv_local + 8, :] = stat.reshape(pieces, 8, 128).astype(bf16)


def place_of(sequence):
    device = sequence // 2
    return device // 2, device % 2, sequence % 2


def scalars_of(ref):
    row = ref[...]
    return [row[0, n] for n in range(row.shape[1])]


def tile_of(x, k, i):
    x = x[8 * (k // 2) : 8 * (k // 2) + 8]
    return jnp.where(i == k % 2, x, pltpu.roll(x, 4, 0))


def merged(old_stat, old_acc, best_new, total_new, acc_new, used, lane8):
    stat, accs = old_stat, []
    for k in range(4):
        best_old, high, low = (old_stat[:, 4 * k + c : 4 * k + c + 1] for c in range(3))
        best = jnp.maximum(best_old, best_new[k])
        first = jnp.exp(best_old - best)
        second = jnp.exp(best_new[k] - best)
        total = (high + low) * first + total_new[k] * second
        accs.append(jnp.where(used, old_acc[k] * first + acc_new[k] * second, old_acc[k]))
        rest = rounded(total)
        stat = jnp.where(used & (lane8 == 4 * k), best, stat)
        stat = jnp.where(used & (lane8 == 4 * k + 1), rest, stat)
        stat = jnp.where(used & (lane8 == 4 * k + 2), total - rest, stat)
    return stat, accs


def part_at(ref, piece):
    return ref[piece, 32:40, :].astype(f32), [
        ref[piece, 8 * k : 8 * k + 8, :].astype(f32) for k in range(4)
    ]


def suffix_kernel(
    ids_ref, len_ref, mine_ref, other_ref, keys_ref, values_ref, part_ref, out_ref, found_ref
):
    del part_ref
    slots, wide, dim = keys_ref.shape
    scale = dim ** (-0.5)
    log2e = 1.4426950408889634
    chunk = 1024
    row = lax.broadcasted_iota(jnp.int32, (16, chunk), 0)
    lane = lax.broadcasted_iota(jnp.int32, (16, chunk), 1)
    position = jnp.where(lane % 4 == row // 4, lane // 4, 1 << 20)
    sub8 = lax.broadcasted_iota(jnp.int32, (8, dim), 0)
    lane8 = lax.broadcasted_iota(jnp.int32, (8, dim), 1)
    my_core = lax.axis_index("core")
    ids, lengths = scalars_of(ids_ref), scalars_of(len_ref)

    def scores_of(s):
        piece, core, i = place_of(ids[s])
        length = lengths[s]
        q = jnp.where(core == my_core, mine_ref[piece].astype(f32), other_ref[piece].astype(f32))
        pairs = []
        for k in (0, 2):
            even, odd = q[8 * k : 8 * k + 8], q[8 * k + 8 : 8 * k + 16]
            even = jnp.where(i == 0, even, pltpu.roll(even, 4, 0))
            odd = jnp.where(i == 0, pltpu.roll(odd, 4, 0), odd)
            pairs.append(jnp.where(sub8 < 4, even, odd))
        q16 = jnp.concatenate(pairs, axis=0).astype(bf16)
        parts = []
        peak = jnp.full((16, 128), negative_fill, f32)
        for c in range(wide // chunk):
            part = nt_dot(q16, keys_ref[s, c * chunk : (c + 1) * chunk, :])
            part = jnp.where(position < length - c * (chunk // 4), part, negative_fill)
            for t in range(chunk // 128):
                peak = jnp.maximum(peak, part[:, 128 * t : 128 * t + 128])
            parts.append(part)
        return parts, rounded(jnp.max(peak, axis=1, keepdims=True) * scale)

    def finish(s, parts, best):
        sums = jnp.zeros((16, 128), f32)
        acc = jnp.zeros((16, dim), f32)
        for c in range(wide // chunk):
            weights = jnp.exp2(parts[c] * (scale * log2e) - best * log2e)
            for t in range(chunk // 128):
                sums = sums + weights[:, 128 * t : 128 * t + 128]
            acc = acc + jnp.dot(
                weights.astype(bf16),
                values_ref[s, c * chunk : (c + 1) * chunk, :],
                preferred_element_type=f32,
            )
        total = jnp.broadcast_to(jnp.sum(sums, axis=1, keepdims=True), (16, dim))
        best = jnp.broadcast_to(best, (16, dim))
        piece, core, i = place_of(ids[s])
        bests, totals, accs = ([tile_of(x, k, i) for k in range(4)] for x in (best, total, acc))
        stat = jnp.zeros((8, dim), f32)
        for k in range(4):
            found_ref[s, 8 * k : 8 * k + 8, :] = accs[k]
            stat = jnp.where(lane8 == 4 * k, bests[k], stat)
            stat = jnp.where(lane8 == 4 * k + 1, totals[k], stat)
        found_ref[s, 32:40, :] = jnp.where(lane8 == 16, ids[s].astype(f32), stat)
        used = (sub8 // 4 == i) & (core == my_core)
        old_stat, old_accs = part_at(out_ref, piece)
        stat, accs = merged(old_stat, old_accs, bests, totals, accs, used, lane8)
        for k in range(4):
            out_ref[piece, 8 * k : 8 * k + 8, :] = accs[k].astype(bf16)
        out_ref[piece, 32:40, :] = stat.astype(bf16)

    ready = scores_of(0)
    for s in range(slots):
        following = scores_of(s + 1) if s + 1 < slots else None
        finish(s, *ready)
        ready = following


def merge_kernel(part_ref, found_ref, out_ref):
    del part_ref
    sub8 = lax.broadcasted_iota(jnp.int32, (8, 128), 0)
    lane8 = lax.broadcasted_iota(jnp.int32, (8, 128), 1)
    results = []
    places = []
    for s in range(found_ref.shape[0]):
        new = found_ref[s, 32:40, :]
        piece, core, i = place_of(new[0, 16].astype(jnp.int32))
        places.append((piece, core))
        bests, totals = ([new[:, 4 * k + c : 4 * k + c + 1] for k in range(4)] for c in range(2))
        accs = [found_ref[s, 8 * k : 8 * k + 8, :] for k in range(4)]
        old_stat, old_accs = part_at(out_ref, piece)
        results.append(merged(old_stat, old_accs, bests, totals, accs, sub8 // 4 == i, lane8))
    for s, (stat, accs) in enumerate(results):
        piece, core = places[s]

        @pl.when(core == lax.axis_index("core"))
        def _():
            for k in range(4):
                out_ref[piece, 8 * k : 8 * k + 8, :] = accs[k].astype(bf16)
            out_ref[piece, 32:40, :] = stat.astype(bf16)


def combine_kernel(got_ref, out_hbm, out_ref, sems):
    copies = []
    count = got_ref.shape[0] // 2
    sub8 = lax.broadcasted_iota(jnp.int32, (8, 128), 0)
    for half in range(2):
        at = slice(half * count, (half + 1) * count)
        stat = got_ref[at, 32:40, :].astype(f32)
        top = jnp.max(stat, axis=0, keepdims=True)
        factor = jnp.exp(stat - top)
        total = pltpu.roll(stat, 127, 2) + pltpu.roll(stat, 126, 2)
        factor = factor / jnp.sum(factor * total, axis=0, keepdims=True)
        rows = []
        for k in range(4):
            acc = got_ref[at, 8 * k : 8 * k + 8, :].astype(f32)
            rows.append(jnp.sum(acc * factor[:, :, 4 * k : 4 * k + 1], axis=0))
        for k in (0, 2):
            base = 16 * half + 4 * k
            turned = pltpu.roll(rows[k + 1], 4, 0)
            out_ref[0, base : base + 8, :] = jnp.where(sub8 < 4, rows[k], turned).astype(bf16)
            turned = pltpu.roll(rows[k], 4, 0)
            out_ref[1, base : base + 8, :] = jnp.where(sub8 < 4, turned, rows[k + 1]).astype(bf16)
        part = (slice(None), slice(16 * half, 16 * half + 16))
        copies.append(pltpu.make_async_copy(out_ref.at[part], out_hbm.at[part], sems.at[half]))
        copies[half].start()
    for copy in copies:
        copy.wait()


def shards(
    queries, prefix_keys, prefix_values, suffix_keys, suffix_values, suffix_lengths, slot_sequence
):
    kv_count = lax.axis_size("kv")
    m_count = lax.axis_size("m")
    per_device, head_count, dim = queries.shape
    local_heads = head_count // kv_count
    kv_local = prefix_keys.shape[1]
    pieces = kv_count * m_count
    slots, suffix_len = suffix_keys.shape[:2]
    swap = [(0, 1), (1, 0)]

    def across(x):
        return lax.ppermute(x, "core", swap)

    def exchange(x):
        return lax.all_to_all(x, ("kv", "m"), split_axis=0, concat_axis=0, tiled=True)

    sent = pl.pallas_call(
        ask_kernel,
        in_specs=[vmem],
        out_specs=vmem,
        out_shape=jax.ShapeDtypeStruct((kv_count, m_count, per_device * local_heads, dim), bf16),
        cost_estimate=pl.CostEstimate(flops=10**11, transcendentals=0, bytes_accessed=2**28),
        compiler_params=limit(4),
        name="ask",
    )(queries)
    there = across(prefix_keys), across(prefix_values)
    mine = exchange(sent.reshape(pieces, per_device * local_heads, dim))
    other = across(mine)

    part = pl.pallas_call(
        prefix_kernel,
        in_specs=[vmem] * 5,
        out_specs=vmem,
        out_shape=jax.ShapeDtypeStruct((pieces, per_device * local_heads + 8, dim), bf16),
        cost_estimate=pl.CostEstimate(flops=10**9, transcendentals=0, bytes_accessed=2**21),
        scratch_shapes=[pltpu.VMEM((2, 2, prefix_keys.shape[0] * kv_local, dim), f32)],
        compiler_params=limit(6),
        name="prefix",
    )(mine, prefix_keys, prefix_values, *there)

    keys = suffix_keys.reshape(slots, suffix_len * kv_local, dim)
    values = suffix_values.reshape(slots, suffix_len * kv_local, dim)
    part, found = pl.pallas_call(
        suffix_kernel,
        in_specs=[vmem] * 7,
        out_specs=[vmem] * 2,
        out_shape=[
            jax.ShapeDtypeStruct(part.shape, bf16),
            jax.ShapeDtypeStruct((slots, per_device * local_heads + 8, dim), f32),
        ],
        input_output_aliases={6: 0},
        cost_estimate=pl.CostEstimate(flops=10**9, transcendentals=0, bytes_accessed=2**21),
        compiler_params=limit(4),
        name="suffix",
    )(*(x.reshape(1, slots) for x in (slot_sequence, suffix_lengths)), mine, other, keys, values, part)
    found_there = across(found)

    part = pl.pallas_call(
        merge_kernel,
        in_specs=[vmem] * 2,
        out_specs=vmem,
        out_shape=jax.ShapeDtypeStruct(part.shape, bf16),
        input_output_aliases={0: 0},
        compiler_params=limit(4),
        name="merge",
    )(part, found_there)

    got = exchange(part)
    return pl.pallas_call(
        combine_kernel,
        in_specs=[vmem],
        out_specs=in_hbm,
        out_shape=jax.ShapeDtypeStruct(queries.shape, bf16),
        scratch_shapes=[pltpu.VMEM(queries.shape, bf16), pltpu.SemaphoreType.DMA((2,))],
        compiler_params=limit(4),
        name="combine",
    )(got)


def solution(mesh):
    kv, batch = (mesh.shape[a] for a in ("kv", "batch"))
    fine = Mesh(mesh.devices.reshape(kv, batch // 2, 2), ("kv", "m", "core"))
    rows, positions = ("kv", "m", "core"), ("m", "core")
    return jax.shard_map(
        shards,
        mesh=fine,
        in_specs=(
            P(rows, None, None),
            P(positions, "kv", None),
            P(positions, "kv", None),
            P(positions, None, "kv", None),
            P(positions, None, "kv", None),
            P(positions),
            P(positions),
        ),
        out_specs=P(rows, None, None),
        check_vma=False,
    )
```

```python
import jax
import jax.numpy as jnp
from jax import lax
from jax.experimental import pallas as pl
from jax.experimental.pallas import tpu as pltpu
from jax.sharding import Mesh
from jax.sharding import PartitionSpec as P

negative_fill = -1e30
f32 = jnp.float32
bf16 = jnp.bfloat16
vmem = pl.BlockSpec(memory_space=pltpu.VMEM)


def limit(mib):
    return pltpu.CompilerParams(vmem_limit_bytes=mib << 20)


def rounded(x):
    return x.astype(bf16).astype(f32)


def nt_dot(a, b):
    return lax.dot_general(a, b, (((1,), (1,)), ((), ())), preferred_element_type=f32)


def scalars_of(ref):
    row = ref[...]
    return [row[0, n] for n in range(row.shape[1])]


def ask_kernel(queries_ref, out_ref):
    groups, copies = out_ref.shape[:2]
    sub8 = lax.broadcasted_iota(jnp.int32, (8, out_ref.shape[3]), 0)
    for g in range(groups):
        tiles = []
        for k in (0, 2):
            base = 16 * g + 4 * k
            one = queries_ref[0, base : base + 8, :].astype(f32)
            two = queries_ref[1, base : base + 8, :].astype(f32)
            tiles.append(jnp.where(sub8 < 4, one, pltpu.roll(two, 4, 0)))
            tiles.append(jnp.where(sub8 < 4, pltpu.roll(one, 4, 0), two))
        piece = jnp.concatenate(tiles, axis=0).astype(bf16)
        for c in range(copies):
            out_ref[g, c] = piece


def stat_with(stat, lane, k, best, total):
    high = rounded(total)
    stat = jnp.where(lane == 4 * k, best, stat)
    stat = jnp.where(lane == 4 * k + 1, high, stat)
    return jnp.where(lane == 4 * k + 2, total - high, stat)


def prefix_kernel(q_ref, k0_ref, v0_ref, k1_ref, v1_ref, out_ref, wide_ref):
    pieces = q_ref.shape[0]
    positions, kv_local, dim = k0_ref.shape
    scale = dim ** (-0.5)
    rows = pieces * 8
    lane = lax.broadcasted_iota(jnp.int32, (rows, 128), 1)
    stat = jnp.zeros((rows, 128), f32)
    for n, pair in enumerate(((k0_ref, k1_ref), (v0_ref, v1_ref))):
        for c, ref in enumerate(pair):
            wide_ref[n, c] = ref[...].astype(f32).reshape(positions * kv_local, dim)

    def block_of(n, k):
        parts = [wide_ref[n, c, pl.ds(k, positions, stride=kv_local), :] for c in range(2)]
        return jnp.concatenate(parts, axis=0).astype(bf16)

    for k in range(kv_local):
        q = q_ref[:, 8 * k : 8 * k + 8, :].astype(f32).reshape(rows, dim).astype(bf16)
        keys, values = block_of(0, k), block_of(1, k)
        scores = nt_dot(q, keys) * scale
        best = rounded(jnp.max(scores, axis=1, keepdims=True))
        weights = jnp.exp(scores - best)
        total = jnp.sum(weights, axis=1, keepdims=True)
        acc = jnp.dot(weights.astype(bf16), values, preferred_element_type=f32)
        out_ref[:, 8 * k : 8 * k + 8, :] = acc.reshape(pieces, 8, dim).astype(bf16)
        stat = stat_with(stat, lane, k, best, total)
    out_ref[:, 8 * kv_local : 8 * kv_local + 8, :] = stat.reshape(pieces, 8, 128).astype(bf16)


def place_of(sequence):
    device = sequence // 2
    return device // 2, device % 2, sequence % 2


def tile_of(x, k, i):
    x = x[8 * (k // 2) : 8 * (k // 2) + 8]
    return jnp.where(i == k % 2, x, pltpu.roll(x, 4, 0))


def merged(piece_ref, piece, new, used):
    lane = lax.broadcasted_iota(jnp.int32, (8, 128), 1)
    old_stat, new_stat = piece_ref[piece, 32:40, :].astype(f32), new[32:40]
    stat, tiles = jnp.zeros((8, 128), f32), []
    for k in range(4):
        at = slice(8 * k, 8 * k + 8)
        best_old, high, low = (old_stat[:, 4 * k + c : 4 * k + c + 1] for c in range(3))
        best_new, total_new = (new_stat[:, 4 * k + c : 4 * k + c + 1] for c in range(2))
        best = jnp.maximum(best_old, best_new)
        first, second = jnp.exp(best_old - best), jnp.exp(best_new - best)
        old = piece_ref[piece, at, :].astype(f32)
        tiles.append(jnp.where(used, old * first + new[at] * second, old))
        stat = stat_with(stat, lane, k, best, (high + low) * first + total_new * second)
    return [*tiles, jnp.where(used, stat, old_stat)]


def suffix_kernel(ids_ref, len_ref, mine_ref, other_ref, keys_ref, values_ref, found_ref):
    slots, wide, dim = keys_ref.shape
    scale = dim ** (-0.5)
    log2e = 1.4426950408889634
    chunk = 1024
    row = lax.broadcasted_iota(jnp.int32, (16, chunk), 0)
    lane = lax.broadcasted_iota(jnp.int32, (16, chunk), 1)
    position = jnp.where(lane % 4 == row // 4, lane // 4, 1 << 20)
    sub8 = lax.broadcasted_iota(jnp.int32, (8, dim), 0)
    lane8 = lax.broadcasted_iota(jnp.int32, (8, dim), 1)
    my_core = lax.axis_index("core")
    ids, lengths = scalars_of(ids_ref), scalars_of(len_ref)

    def scores_of(s):
        piece, core, i = place_of(ids[s])
        length = lengths[s]
        q = jnp.where(core == my_core, mine_ref[piece].astype(f32), other_ref[piece].astype(f32))
        pairs = []
        for k in (0, 2):
            even, odd = q[8 * k : 8 * k + 8], q[8 * k + 8 : 8 * k + 16]
            even = jnp.where(i == 0, even, pltpu.roll(even, 4, 0))
            odd = jnp.where(i == 0, pltpu.roll(odd, 4, 0), odd)
            pairs.append(jnp.where(sub8 < 4, even, odd))
        q16 = jnp.concatenate(pairs, axis=0).astype(bf16)
        parts = []
        peak = jnp.full((16, 128), negative_fill, f32)
        for c in range(wide // chunk):
            part = nt_dot(q16, keys_ref[s, c * chunk : (c + 1) * chunk, :])
            part = jnp.where(position < length - c * (chunk // 4), part, negative_fill)
            for t in range(chunk // 128):
                peak = jnp.maximum(peak, part[:, 128 * t : 128 * t + 128])
            parts.append(part)
        return parts, rounded(jnp.max(peak, axis=1, keepdims=True) * scale)

    def finish(s, parts, best):
        sums = jnp.zeros((16, 128), f32)
        acc = jnp.zeros((16, dim), f32)
        for c in range(wide // chunk):
            weights = jnp.exp2(parts[c] * (scale * log2e) - best * log2e)
            for t in range(chunk // 128):
                sums = sums + weights[:, 128 * t : 128 * t + 128]
            acc = acc + jnp.dot(
                weights.astype(bf16),
                values_ref[s, c * chunk : (c + 1) * chunk, :],
                preferred_element_type=f32,
            )
        total = jnp.broadcast_to(jnp.sum(sums, axis=1, keepdims=True), (16, dim))
        best = jnp.broadcast_to(best, (16, dim))
        _, _, i = place_of(ids[s])
        stat = jnp.where(lane8 == 127, ids[s].astype(f32), jnp.zeros((8, dim), f32))
        for k in range(4):
            found_ref[s, 8 * k : 8 * k + 8, :] = tile_of(acc, k, i)
            stat = jnp.where(lane8 == 4 * k, tile_of(best, k, i), stat)
            stat = jnp.where(lane8 == 4 * k + 1, tile_of(total, k, i), stat)
        found_ref[s, 32:40, :] = stat

    ready = scores_of(0)
    for s in range(slots):
        following = scores_of(s + 1) if s + 1 < slots else None
        finish(s, *ready)
        ready = following


def merge_kernel(part_ref, mine_ref, other_ref, out_ref):
    del part_ref
    slots = mine_ref.shape[0]
    sub8 = lax.broadcasted_iota(jnp.int32, (8, 128), 0)
    my_core = lax.axis_index("core")
    places = []
    for ref in (mine_ref, other_ref):
        numbers = [ref[s, 32:40, :][0, 127].astype(jnp.int32) for s in range(slots)]
        places.append([place_of(number) for number in numbers])
    for ref, where in zip((mine_ref, other_ref), places):
        results = [
            merged(out_ref, piece, ref[s], sub8 // 4 == i) for s, (piece, _, i) in enumerate(where)
        ]
        for (piece, core, _), tiles in zip(where, results):

            @pl.when(core == my_core)
            def _():
                for k, tile in enumerate(tiles):
                    out_ref[piece, 8 * k : 8 * k + 8, :] = tile.astype(bf16)


def combine_kernel(got_ref, out_ref):
    count = got_ref.shape[0] // 2
    sub8 = lax.broadcasted_iota(jnp.int32, (8, 128), 0)
    for half in range(2):
        at = slice(half * count, (half + 1) * count)
        stat = got_ref[at, 32:40, :].astype(f32)
        factor = jnp.exp(stat - jnp.max(stat, axis=0, keepdims=True))
        total = pltpu.roll(stat, 127, 2) + pltpu.roll(stat, 126, 2)
        inverse = 1.0 / jnp.sum(factor * total, axis=0)
        rows = []
        for k in range(4):
            acc = got_ref[at, 8 * k : 8 * k + 8, :].astype(f32)
            acc = jnp.sum(acc * factor[:, :, 4 * k : 4 * k + 1], axis=0)
            rows.append(acc * inverse[:, 4 * k : 4 * k + 1])
        for k in (0, 2):
            base = 16 * half + 4 * k
            turned = pltpu.roll(rows[k + 1], 4, 0)
            out_ref[0, base : base + 8, :] = jnp.where(sub8 < 4, rows[k], turned).astype(bf16)
            turned = pltpu.roll(rows[k], 4, 0)
            out_ref[1, base : base + 8, :] = jnp.where(sub8 < 4, turned, rows[k + 1]).astype(bf16)


def shards(
    queries, prefix_keys, prefix_values, suffix_keys, suffix_values, suffix_lengths, slot_sequence
):
    kv_count = lax.axis_size("kv")
    m_count = lax.axis_size("m")
    per_device, head_count, dim = queries.shape
    local_heads = head_count // kv_count
    kv_local = prefix_keys.shape[1]
    pieces = kv_count * m_count
    slots, suffix_len = suffix_keys.shape[:2]
    swap = [(0, 1), (1, 0)]

    def across(x):
        return lax.ppermute(x, "core", swap)

    def exchange(x):
        return lax.all_to_all(x, ("kv", "m"), split_axis=0, concat_axis=0, tiled=True)

    sent = pl.pallas_call(
        ask_kernel,
        in_specs=[vmem],
        out_specs=vmem,
        out_shape=jax.ShapeDtypeStruct((kv_count, m_count, per_device * local_heads, dim), bf16),
        cost_estimate=pl.CostEstimate(flops=10**11, transcendentals=0, bytes_accessed=2**28),
        compiler_params=limit(4),
        name="ask",
    )(queries)
    mine = exchange(sent.reshape(pieces, per_device * local_heads, dim))
    other = across(mine)
    there = across(prefix_keys), across(prefix_values)

    keys = suffix_keys.reshape(slots, suffix_len * kv_local, dim)
    values = suffix_values.reshape(slots, suffix_len * kv_local, dim)
    found = pl.pallas_call(
        suffix_kernel,
        in_specs=[vmem] * 6,
        out_specs=vmem,
        out_shape=jax.ShapeDtypeStruct((slots, per_device * local_heads + 8, dim), f32),
        cost_estimate=pl.CostEstimate(flops=10**9, transcendentals=0, bytes_accessed=2**21),
        compiler_params=limit(4),
        name="suffix",
    )(*(x.reshape(1, slots) for x in (slot_sequence, suffix_lengths)), mine, other, keys, values)
    found_there = across(found)

    part = pl.pallas_call(
        prefix_kernel,
        in_specs=[vmem] * 5,
        out_specs=vmem,
        out_shape=jax.ShapeDtypeStruct((pieces, per_device * local_heads + 8, dim), bf16),
        scratch_shapes=[pltpu.VMEM((2, 2, prefix_keys.shape[0] * kv_local, dim), f32)],
        cost_estimate=pl.CostEstimate(flops=10**9, transcendentals=0, bytes_accessed=2**21),
        compiler_params=limit(6),
        name="prefix",
    )(mine, prefix_keys, prefix_values, *there)
    part = pl.pallas_call(
        merge_kernel,
        in_specs=[vmem] * 3,
        out_specs=vmem,
        out_shape=jax.ShapeDtypeStruct(part.shape, bf16),
        input_output_aliases={0: 0},
        compiler_params=limit(4),
        name="merge",
    )(part, found, found_there)

    got = exchange(part)
    return pl.pallas_call(
        combine_kernel,
        in_specs=[vmem],
        out_specs=vmem,
        out_shape=jax.ShapeDtypeStruct(queries.shape, bf16),
        compiler_params=limit(4),
        name="combine",
    )(got)


def solution(mesh):
    kv, batch = (mesh.shape[a] for a in ("kv", "batch"))
    fine = Mesh(mesh.devices.reshape(kv, batch // 2, 2), ("kv", "m", "core"))
    rows, positions = ("kv", "m", "core"), ("m", "core")
    return jax.shard_map(
        shards,
        mesh=fine,
        in_specs=(
            P(rows, None, None),
            P(positions, "kv", None),
            P(positions, "kv", None),
            P(positions, None, "kv", None),
            P(positions, None, "kv", None),
            P(positions),
            P(positions),
        ),
        out_specs=P(rows, None, None),
        check_vma=False,
    )
```

```python
import jax
import jax.numpy as jnp
from jax import lax
from jax.experimental import pallas as pl
from jax.experimental.pallas import tpu as pltpu
from jax.sharding import Mesh
from jax.sharding import PartitionSpec as P

negative_fill = -1e30
f32 = jnp.float32
bf16 = jnp.bfloat16
vmem = pl.BlockSpec(memory_space=pltpu.VMEM)


def limit(mib):
    return pltpu.CompilerParams(vmem_limit_bytes=mib << 20)


def rounded(x):
    return x.astype(bf16).astype(f32)


def nt_dot(a, b):
    return lax.dot_general(a, b, (((1,), (1,)), ((), ())), preferred_element_type=f32)


def scalars_of(ref):
    row = ref[...]
    return [row[0, n] for n in range(row.shape[1])]


def first_kernel(out_ref):
    out_ref[...] = jnp.zeros(out_ref.shape, out_ref.dtype)


def ask_kernel(queries_ref, first_ref, out_ref):
    del first_ref
    groups, copies = out_ref.shape[:2]
    sub8 = lax.broadcasted_iota(jnp.int32, (8, out_ref.shape[3]), 0)
    for g in range(groups):
        tiles = []
        for k in (0, 2):
            base = 16 * g + 4 * k
            one = queries_ref[0, base : base + 8, :].astype(f32)
            two = queries_ref[1, base : base + 8, :].astype(f32)
            tiles.append(jnp.where(sub8 < 4, one, pltpu.roll(two, 4, 0)))
            tiles.append(jnp.where(sub8 < 4, pltpu.roll(one, 4, 0), two))
        piece = jnp.concatenate(tiles, axis=0).astype(bf16)
        for c in range(copies):
            out_ref[g, c] = piece


def stat_with(stat, lane, k, best, total):
    high = rounded(total)
    stat = jnp.where(lane == 4 * k, best, stat)
    stat = jnp.where(lane == 4 * k + 1, high, stat)
    return jnp.where(lane == 4 * k + 2, total - high, stat)


def prefix_kernel(q_ref, k0_ref, v0_ref, k1_ref, v1_ref, out_ref, wide_ref):
    pieces = q_ref.shape[0]
    positions, kv_local, dim = k0_ref.shape
    scale = dim ** (-0.5)
    rows = pieces * 8
    lane = lax.broadcasted_iota(jnp.int32, (rows, 128), 1)
    stat = jnp.zeros((rows, 128), f32)
    for n, pair in enumerate(((k0_ref, k1_ref), (v0_ref, v1_ref))):
        for c, ref in enumerate(pair):
            wide_ref[n, c] = ref[...].astype(f32).reshape(positions * kv_local, dim)

    def block_of(n, k):
        parts = [wide_ref[n, c, pl.ds(k, positions, stride=kv_local), :] for c in range(2)]
        return jnp.concatenate(parts, axis=0).astype(bf16)

    for k in range(kv_local):
        q = q_ref[:, 8 * k : 8 * k + 8, :].astype(f32).reshape(rows, dim).astype(bf16)
        keys, values = block_of(0, k), block_of(1, k)
        scores = nt_dot(q, keys) * scale
        best = rounded(jnp.max(scores, axis=1, keepdims=True))
        weights = jnp.exp(scores - best)
        total = jnp.sum(weights, axis=1, keepdims=True)
        acc = jnp.dot(weights.astype(bf16), values, preferred_element_type=f32)
        out_ref[:, 8 * k : 8 * k + 8, :] = acc.reshape(pieces, 8, dim).astype(bf16)
        stat = stat_with(stat, lane, k, best, total)
    out_ref[:, 8 * kv_local : 8 * kv_local + 8, :] = stat.reshape(pieces, 8, 128).astype(bf16)


def place_of(sequence):
    device = sequence // 2
    return device // 2, device % 2, sequence % 2


def tile_of(x, k, i):
    x = x[8 * (k // 2) : 8 * (k // 2) + 8]
    return jnp.where(i == k % 2, x, pltpu.roll(x, 4, 0))


def merged(piece_ref, piece, new, used):
    lane = lax.broadcasted_iota(jnp.int32, (8, 128), 1)
    old_stat, new_stat = piece_ref[piece, 32:40, :].astype(f32), new[32:40]
    stat, tiles = jnp.zeros((8, 128), f32), []
    for k in range(4):
        at = slice(8 * k, 8 * k + 8)
        best_old, high, low = (old_stat[:, 4 * k + c : 4 * k + c + 1] for c in range(3))
        best_new, total_new = (new_stat[:, 4 * k + c : 4 * k + c + 1] for c in range(2))
        best = jnp.maximum(best_old, best_new)
        first, second = jnp.exp(best_old - best), jnp.exp(best_new - best)
        old = piece_ref[piece, at, :].astype(f32)
        tiles.append(jnp.where(used, old * first + new[at] * second, old))
        stat = stat_with(stat, lane, k, best, (high + low) * first + total_new * second)
    return [*tiles, jnp.where(used, stat, old_stat)]


def reached_kernel(mine_ref, out_ref):
    out_ref[...] = mine_ref[0, :8, :]


def pick_kernel(ids_ref, mine_ref, reached_ref, out_ref):
    del reached_ref
    for s, sequence in enumerate(scalars_of(ids_ref)):
        out_ref[s] = mine_ref[place_of(sequence)[0]]


def suffix_kernel(ids_ref, len_ref, mine_ref, other_ref, keys_ref, values_ref, found_ref):
    slots, wide, dim = keys_ref.shape
    scale = dim ** (-0.5)
    log2e = 1.4426950408889634
    chunk = 1024
    row = lax.broadcasted_iota(jnp.int32, (16, chunk), 0)
    lane = lax.broadcasted_iota(jnp.int32, (16, chunk), 1)
    position = jnp.where(lane % 4 == row // 4, lane // 4, 1 << 20)
    sub8 = lax.broadcasted_iota(jnp.int32, (8, dim), 0)
    lane8 = lax.broadcasted_iota(jnp.int32, (8, dim), 1)
    my_core = lax.axis_index("core")
    ids, lengths = scalars_of(ids_ref), scalars_of(len_ref)

    def scores_of(s):
        piece, core, i = place_of(ids[s])
        length = lengths[s]
        q = jnp.where(core == my_core, mine_ref[piece].astype(f32), other_ref[s].astype(f32))
        pairs = []
        for k in (0, 2):
            even, odd = q[8 * k : 8 * k + 8], q[8 * k + 8 : 8 * k + 16]
            even = jnp.where(i == 0, even, pltpu.roll(even, 4, 0))
            odd = jnp.where(i == 0, pltpu.roll(odd, 4, 0), odd)
            pairs.append(jnp.where(sub8 < 4, even, odd))
        q16 = jnp.concatenate(pairs, axis=0).astype(bf16)
        parts = []
        peak = jnp.full((16, 128), negative_fill, f32)
        for c in range(wide // chunk):
            part = nt_dot(q16, keys_ref[s, c * chunk : (c + 1) * chunk, :])
            part = jnp.where(position < length - c * (chunk // 4), part, negative_fill)
            for t in range(chunk // 128):
                peak = jnp.maximum(peak, part[:, 128 * t : 128 * t + 128])
            parts.append(part)
        return parts, rounded(jnp.max(peak, axis=1, keepdims=True) * scale)

    def finish(s, parts, best):
        sums = jnp.zeros((16, 128), f32)
        acc = jnp.zeros((16, dim), f32)
        for c in range(wide // chunk):
            weights = jnp.exp2(parts[c] * (scale * log2e) - best * log2e)
            for t in range(chunk // 128):
                sums = sums + weights[:, 128 * t : 128 * t + 128]
            acc = acc + jnp.dot(
                weights.astype(bf16),
                values_ref[s, c * chunk : (c + 1) * chunk, :],
                preferred_element_type=f32,
            )
        total = jnp.broadcast_to(jnp.sum(sums, axis=1, keepdims=True), (16, dim))
        best = jnp.broadcast_to(best, (16, dim))
        _, _, i = place_of(ids[s])
        stat = jnp.where(lane8 == 127, ids[s].astype(f32), jnp.zeros((8, dim), f32))
        for k in range(4):
            found_ref[s, 8 * k : 8 * k + 8, :] = tile_of(acc, k, i)
            stat = jnp.where(lane8 == 4 * k, tile_of(best, k, i), stat)
            stat = jnp.where(lane8 == 4 * k + 1, tile_of(total, k, i), stat)
        found_ref[s, 32:40, :] = stat

    ready = scores_of(0)
    for s in range(slots):
        following = scores_of(s + 1) if s + 1 < slots else None
        finish(s, *ready)
        ready = following


def merge_kernel(part_ref, mine_ref, other_ref, out_ref):
    del part_ref
    slots = mine_ref.shape[0]
    sub8 = lax.broadcasted_iota(jnp.int32, (8, 128), 0)
    my_core = lax.axis_index("core")
    places = []
    for ref in (mine_ref, other_ref):
        numbers = [ref[s, 32:40, :][0, 127].astype(jnp.int32) for s in range(slots)]
        places.append([place_of(number) for number in numbers])
    for ref, where in zip((mine_ref, other_ref), places):
        results = [
            merged(out_ref, piece, ref[s], sub8 // 4 == i) for s, (piece, _, i) in enumerate(where)
        ]
        for (piece, core, _), tiles in zip(where, results):

            @pl.when(core == my_core)
            def _():
                for k, tile in enumerate(tiles):
                    out_ref[piece, 8 * k : 8 * k + 8, :] = tile.astype(bf16)


def combine_kernel(got_ref, out_ref):
    count = got_ref.shape[0] // 2
    sub8 = lax.broadcasted_iota(jnp.int32, (8, 128), 0)
    for half in range(2):
        at = slice(half * count, (half + 1) * count)
        stat = got_ref[at, 32:40, :].astype(f32)
        factor = jnp.exp(stat - jnp.max(stat, axis=0, keepdims=True))
        total = pltpu.roll(stat, 127, 2) + pltpu.roll(stat, 126, 2)
        inverse = 1.0 / jnp.sum(factor * total, axis=0)
        rows = []
        for k in range(4):
            acc = got_ref[at, 8 * k : 8 * k + 8, :].astype(f32)
            acc = jnp.sum(acc * factor[:, :, 4 * k : 4 * k + 1], axis=0)
            rows.append(acc * inverse[:, 4 * k : 4 * k + 1])
        for k in (0, 2):
            base = 16 * half + 4 * k
            turned = pltpu.roll(rows[k + 1], 4, 0)
            out_ref[0, base : base + 8, :] = jnp.where(sub8 < 4, rows[k], turned).astype(bf16)
            turned = pltpu.roll(rows[k], 4, 0)
            out_ref[1, base : base + 8, :] = jnp.where(sub8 < 4, turned, rows[k + 1]).astype(bf16)


def shards(
    queries, prefix_keys, prefix_values, suffix_keys, suffix_values, suffix_lengths, slot_sequence
):
    kv_count = lax.axis_size("kv")
    m_count = lax.axis_size("m")
    per_device, head_count, dim = queries.shape
    local_heads = head_count // kv_count
    kv_local = prefix_keys.shape[1]
    pieces = kv_count * m_count
    slots, suffix_len = suffix_keys.shape[:2]
    swap = [(0, 1), (1, 0)]

    def across(x):
        return lax.ppermute(x, "core", swap)

    def exchange(x):
        return lax.all_to_all(x, ("kv", "m"), split_axis=0, concat_axis=0, tiled=True)

    first = pl.pallas_call(
        first_kernel,
        out_specs=vmem,
        out_shape=jax.ShapeDtypeStruct((8, 128), f32),
        cost_estimate=pl.CostEstimate(flops=10**11, transcendentals=0, bytes_accessed=2**28),
        compiler_params=limit(1),
        name="first",
    )()
    sent = pl.pallas_call(
        ask_kernel,
        in_specs=[vmem] * 2,
        out_specs=vmem,
        out_shape=jax.ShapeDtypeStruct((kv_count, m_count, per_device * local_heads, dim), bf16),
        compiler_params=limit(4),
        name="ask",
    )(queries, first)
    told, _ = lax.optimization_barrier((slot_sequence, first))
    ids_there = across(told)
    mine = exchange(sent.reshape(pieces, per_device * local_heads, dim))
    reached = pl.pallas_call(
        reached_kernel,
        in_specs=[vmem],
        out_specs=vmem,
        out_shape=jax.ShapeDtypeStruct((8, dim), bf16),
        compiler_params=limit(1),
        name="reached",
    )(mine)
    picked = pl.pallas_call(
        pick_kernel,
        in_specs=[vmem] * 3,
        out_specs=vmem,
        out_shape=jax.ShapeDtypeStruct((slots, per_device * local_heads, dim), bf16),
        compiler_params=limit(1),
        name="pick",
    )(ids_there.reshape(1, slots), mine, reached)
    other = across(picked)
    there = across(prefix_keys), across(prefix_values)

    keys = suffix_keys.reshape(slots, suffix_len * kv_local, dim)
    values = suffix_values.reshape(slots, suffix_len * kv_local, dim)
    found = pl.pallas_call(
        suffix_kernel,
        in_specs=[vmem] * 6,
        out_specs=vmem,
        out_shape=jax.ShapeDtypeStruct((slots, per_device * local_heads + 8, dim), f32),
        cost_estimate=pl.CostEstimate(flops=10**9, transcendentals=0, bytes_accessed=2**21),
        compiler_params=limit(4),
        name="suffix",
    )(*(x.reshape(1, slots) for x in (slot_sequence, suffix_lengths)), mine, other, keys, values)
    found_there = across(found)

    part = pl.pallas_call(
        prefix_kernel,
        in_specs=[vmem] * 5,
        out_specs=vmem,
        out_shape=jax.ShapeDtypeStruct((pieces, per_device * local_heads + 8, dim), bf16),
        scratch_shapes=[pltpu.VMEM((2, 2, prefix_keys.shape[0] * kv_local, dim), f32)],
        cost_estimate=pl.CostEstimate(flops=10**9, transcendentals=0, bytes_accessed=2**21),
        compiler_params=limit(6),
        name="prefix",
    )(mine, prefix_keys, prefix_values, *there)
    part = pl.pallas_call(
        merge_kernel,
        in_specs=[vmem] * 3,
        out_specs=vmem,
        out_shape=jax.ShapeDtypeStruct(part.shape, bf16),
        input_output_aliases={0: 0},
        compiler_params=limit(4),
        name="merge",
    )(part, found, found_there)

    got = exchange(part)
    return pl.pallas_call(
        combine_kernel,
        in_specs=[vmem],
        out_specs=vmem,
        out_shape=jax.ShapeDtypeStruct(queries.shape, bf16),
        compiler_params=limit(4),
        name="combine",
    )(got)


def solution(mesh):
    kv, batch = (mesh.shape[a] for a in ("kv", "batch"))
    fine = Mesh(mesh.devices.reshape(kv, batch // 2, 2), ("kv", "m", "core"))
    rows, positions = ("kv", "m", "core"), ("m", "core")
    return jax.shard_map(
        shards,
        mesh=fine,
        in_specs=(
            P(rows, None, None),
            P(positions, "kv", None),
            P(positions, "kv", None),
            P(positions, None, "kv", None),
            P(positions, None, "kv", None),
            P(positions),
            P(positions),
        ),
        out_specs=P(rows, None, None),
        check_vma=False,
    )
```

```python
import jax
import jax.numpy as jnp
from jax import lax
from jax.experimental import pallas as pl
from jax.experimental.pallas import tpu as pltpu
from jax.sharding import Mesh
from jax.sharding import PartitionSpec as P

negative_fill = -1e30
f32 = jnp.float32
bf16 = jnp.bfloat16
vmem = pl.BlockSpec(memory_space=pltpu.VMEM)


def limit(mib):
    return pltpu.CompilerParams(vmem_limit_bytes=mib << 20)


def rounded(x):
    return x.astype(bf16).astype(f32)


def nt_dot(a, b):
    return lax.dot_general(a, b, (((1,), (1,)), ((), ())), preferred_element_type=f32)


def scalars_of(ref):
    row = ref[...]
    return [row[0, n] for n in range(row.shape[1])]


def first_kernel(out_ref):
    out_ref[...] = jnp.zeros(out_ref.shape, out_ref.dtype)


def ask_kernel(queries_ref, first_ref, out_ref):
    del first_ref
    groups, copies = out_ref.shape[:2]
    sub8 = lax.broadcasted_iota(jnp.int32, (8, out_ref.shape[3]), 0)
    for g in range(groups):
        tiles = []
        for k in (0, 2):
            base = 16 * g + 4 * k
            one = queries_ref[0, base : base + 8, :].astype(f32)
            two = queries_ref[1, base : base + 8, :].astype(f32)
            tiles.append(jnp.where(sub8 < 4, one, pltpu.roll(two, 4, 0)))
            tiles.append(jnp.where(sub8 < 4, pltpu.roll(one, 4, 0), two))
        piece = jnp.concatenate(tiles, axis=0).astype(bf16)
        for c in range(copies):
            out_ref[g, c] = piece


def stat_with(stat, lane, k, best, total):
    high = rounded(total)
    stat = jnp.where(lane == 4 * k, best, stat)
    stat = jnp.where(lane == 4 * k + 1, high, stat)
    return jnp.where(lane == 4 * k + 2, total - high, stat)


def prefix_kernel(q_ref, k0_ref, v0_ref, k1_ref, v1_ref, out_ref, wide_ref):
    pieces = q_ref.shape[0]
    positions, kv_local, dim = k0_ref.shape
    scale = dim ** (-0.5)
    log2e = 1.4426950408889634
    rows = pieces * 8
    lane = lax.broadcasted_iota(jnp.int32, (rows, 128), 1)
    stat = jnp.zeros((rows, 128), f32)
    for n, pair in enumerate(((k0_ref, k1_ref), (v0_ref, v1_ref))):
        for c, ref in enumerate(pair):
            wide_ref[n, c] = ref[...].astype(f32).reshape(positions * kv_local, dim)

    def block_of(n, k):
        parts = [wide_ref[n, c, pl.ds(k, positions, stride=kv_local), :] for c in range(2)]
        return jnp.concatenate(parts, axis=0).astype(bf16)

    for k in range(kv_local):
        q = q_ref[:, 8 * k : 8 * k + 8, :].astype(f32).reshape(rows, dim).astype(bf16)
        keys, values = block_of(0, k), block_of(1, k)
        scores = nt_dot(q, keys)
        best = rounded(jnp.max(scores, axis=1, keepdims=True) * scale)
        weights = jnp.exp2(scores * (scale * log2e) - best * log2e)
        total = jnp.sum(weights, axis=1, keepdims=True)
        acc = jnp.dot(weights.astype(bf16), values, preferred_element_type=f32)
        out_ref[:, 8 * k : 8 * k + 8, :] = acc.reshape(pieces, 8, dim).astype(bf16)
        stat = stat_with(stat, lane, k, best, total)
    out_ref[:, 8 * kv_local : 8 * kv_local + 8, :] = stat.reshape(pieces, 8, 128).astype(bf16)


def place_of(sequence):
    device = sequence // 2
    return device // 2, device % 2, sequence % 2


def tile_of(x, k, i):
    x = x[8 * (k // 2) : 8 * (k // 2) + 8]
    return jnp.where(i == k % 2, x, pltpu.roll(x, 4, 0))


def merged(piece_ref, piece, new, used):
    lane = lax.broadcasted_iota(jnp.int32, (8, 128), 1)
    old_stat, new_stat = piece_ref[piece, 32:40, :].astype(f32), new[32:40]
    stat, tiles = jnp.zeros((8, 128), f32), []
    for k in range(4):
        at = slice(8 * k, 8 * k + 8)
        best_old, high, low = (old_stat[:, 4 * k + c : 4 * k + c + 1] for c in range(3))
        best_new, total_new = (new_stat[:, 4 * k + c : 4 * k + c + 1] for c in range(2))
        best = jnp.maximum(best_old, best_new)
        first, second = jnp.exp(best_old - best), jnp.exp(best_new - best)
        old = piece_ref[piece, at, :].astype(f32)
        tiles.append(jnp.where(used, old * first + new[at] * second, old))
        stat = stat_with(stat, lane, k, best, (high + low) * first + total_new * second)
    return [*tiles, jnp.where(used, stat, old_stat)]


def reached_kernel(mine_ref, out_ref):
    out_ref[...] = mine_ref[0, :8, :]


def pick_kernel(ids_ref, mine_ref, reached_ref, out_ref):
    del reached_ref
    for s, sequence in enumerate(scalars_of(ids_ref)):
        out_ref[s] = mine_ref[place_of(sequence)[0]]


def suffix_kernel(ids_ref, len_ref, mine_ref, other_ref, keys_ref, values_ref, found_ref):
    slots, wide, dim = keys_ref.shape
    scale = dim ** (-0.5)
    log2e = 1.4426950408889634
    chunk = 1024
    row = lax.broadcasted_iota(jnp.int32, (16, chunk), 0)
    lane = lax.broadcasted_iota(jnp.int32, (16, chunk), 1)
    position = jnp.where(lane % 4 == row // 4, lane // 4, 1 << 20)
    sub8 = lax.broadcasted_iota(jnp.int32, (8, dim), 0)
    lane8 = lax.broadcasted_iota(jnp.int32, (8, dim), 1)
    my_core = lax.axis_index("core")
    ids, lengths = scalars_of(ids_ref), scalars_of(len_ref)

    def scores_of(s):
        piece, core, i = place_of(ids[s])
        length = lengths[s]
        q = jnp.where(core == my_core, mine_ref[piece].astype(f32), other_ref[s].astype(f32))
        pairs = []
        for k in (0, 2):
            even, odd = q[8 * k : 8 * k + 8], q[8 * k + 8 : 8 * k + 16]
            even = jnp.where(i == 0, even, pltpu.roll(even, 4, 0))
            odd = jnp.where(i == 0, pltpu.roll(odd, 4, 0), odd)
            pairs.append(jnp.where(sub8 < 4, even, odd))
        q16 = jnp.concatenate(pairs, axis=0).astype(bf16)
        parts = []
        peak = jnp.full((16, 128), negative_fill, f32)
        for c in range(wide // chunk):
            part = nt_dot(q16, keys_ref[s, c * chunk : (c + 1) * chunk, :])
            part = jnp.where(position < length - c * (chunk // 4), part, negative_fill)
            for t in range(chunk // 128):
                peak = jnp.maximum(peak, part[:, 128 * t : 128 * t + 128])
            parts.append(part)
        return parts, rounded(jnp.max(peak, axis=1, keepdims=True) * scale)

    def finish(s, parts, best):
        sums = jnp.zeros((16, 128), f32)
        acc = jnp.zeros((16, dim), f32)
        for c in range(wide // chunk):
            weights = jnp.exp2(parts[c] * (scale * log2e) - best * log2e)
            for t in range(chunk // 128):
                sums = sums + weights[:, 128 * t : 128 * t + 128]
            acc = acc + jnp.dot(
                weights.astype(bf16),
                values_ref[s, c * chunk : (c + 1) * chunk, :],
                preferred_element_type=f32,
            )
        total = jnp.broadcast_to(jnp.sum(sums, axis=1, keepdims=True), (16, dim))
        best = jnp.broadcast_to(best, (16, dim))
        _, _, i = place_of(ids[s])
        stat = jnp.where(lane8 == 127, ids[s].astype(f32), jnp.zeros((8, dim), f32))
        for k in range(4):
            found_ref[s, 8 * k : 8 * k + 8, :] = tile_of(acc, k, i)
            stat = jnp.where(lane8 == 4 * k, tile_of(best, k, i), stat)
            stat = jnp.where(lane8 == 4 * k + 1, tile_of(total, k, i), stat)
        found_ref[s, 32:40, :] = stat

    ready = scores_of(0)
    for s in range(slots):
        following = scores_of(s + 1) if s + 1 < slots else None
        finish(s, *ready)
        ready = following


def merge_kernel(part_ref, mine_ref, other_ref, out_ref):
    del part_ref
    slots = mine_ref.shape[0]
    sub8 = lax.broadcasted_iota(jnp.int32, (8, 128), 0)
    my_core = lax.axis_index("core")
    places = []
    for ref in (mine_ref, other_ref):
        numbers = [ref[s, 32:40, :][0, 127].astype(jnp.int32) for s in range(slots)]
        places.append([place_of(number) for number in numbers])
    for ref, where in zip((mine_ref, other_ref), places):
        results = [
            merged(out_ref, piece, ref[s], sub8 // 4 == i) for s, (piece, _, i) in enumerate(where)
        ]
        for (piece, core, _), tiles in zip(where, results):

            @pl.when(core == my_core)
            def _():
                for k, tile in enumerate(tiles):
                    out_ref[piece, 8 * k : 8 * k + 8, :] = tile.astype(bf16)


def combine_kernel(got_ref, out_ref):
    count = got_ref.shape[0] // 2
    sub8 = lax.broadcasted_iota(jnp.int32, (8, 128), 0)
    for half in range(2):
        at = slice(half * count, (half + 1) * count)
        stat = got_ref[at, 32:40, :].astype(f32)
        factor = jnp.exp(stat - jnp.max(stat, axis=0, keepdims=True))
        total = pltpu.roll(stat, 127, 2) + pltpu.roll(stat, 126, 2)
        inverse = 1.0 / jnp.sum(factor * total, axis=0)
        rows = []
        for k in range(4):
            acc = got_ref[at, 8 * k : 8 * k + 8, :].astype(f32)
            acc = jnp.sum(acc * factor[:, :, 4 * k : 4 * k + 1], axis=0)
            rows.append(acc * inverse[:, 4 * k : 4 * k + 1])
        for k in (0, 2):
            base = 16 * half + 4 * k
            turned = pltpu.roll(rows[k + 1], 4, 0)
            out_ref[0, base : base + 8, :] = jnp.where(sub8 < 4, rows[k], turned).astype(bf16)
            turned = pltpu.roll(rows[k], 4, 0)
            out_ref[1, base : base + 8, :] = jnp.where(sub8 < 4, turned, rows[k + 1]).astype(bf16)


def shards(
    queries, prefix_keys, prefix_values, suffix_keys, suffix_values, suffix_lengths, slot_sequence
):
    kv_count = lax.axis_size("kv")
    m_count = lax.axis_size("m")
    per_device, head_count, dim = queries.shape
    local_heads = head_count // kv_count
    kv_local = prefix_keys.shape[1]
    pieces = kv_count * m_count
    slots, suffix_len = suffix_keys.shape[:2]
    swap = [(0, 1), (1, 0)]

    def across(x):
        return lax.ppermute(x, "core", swap)

    def exchange(x):
        return lax.all_to_all(x, ("kv", "m"), split_axis=0, concat_axis=0, tiled=True)

    first = pl.pallas_call(
        first_kernel,
        out_specs=vmem,
        out_shape=jax.ShapeDtypeStruct((8, 128), f32),
        cost_estimate=pl.CostEstimate(flops=10**11, transcendentals=0, bytes_accessed=2**28),
        compiler_params=limit(1),
        name="first",
    )()
    sent = pl.pallas_call(
        ask_kernel,
        in_specs=[vmem] * 2,
        out_specs=vmem,
        out_shape=jax.ShapeDtypeStruct((kv_count, m_count, per_device * local_heads, dim), bf16),
        compiler_params=limit(4),
        name="ask",
    )(queries, first)
    told, _ = lax.optimization_barrier((slot_sequence, first))
    ids_there = across(told)
    mine = exchange(sent.reshape(pieces, per_device * local_heads, dim))
    reached = pl.pallas_call(
        reached_kernel,
        in_specs=[vmem],
        out_specs=vmem,
        out_shape=jax.ShapeDtypeStruct((8, dim), bf16),
        compiler_params=limit(1),
        name="reached",
    )(mine)
    picked = pl.pallas_call(
        pick_kernel,
        in_specs=[vmem] * 3,
        out_specs=vmem,
        out_shape=jax.ShapeDtypeStruct((slots, per_device * local_heads, dim), bf16),
        compiler_params=limit(1),
        name="pick",
    )(ids_there.reshape(1, slots), mine, reached)
    other = across(picked)
    there = across(prefix_keys), across(prefix_values)

    keys = suffix_keys.reshape(slots, suffix_len * kv_local, dim)
    values = suffix_values.reshape(slots, suffix_len * kv_local, dim)
    found = pl.pallas_call(
        suffix_kernel,
        in_specs=[vmem] * 6,
        out_specs=vmem,
        out_shape=jax.ShapeDtypeStruct((slots, per_device * local_heads + 8, dim), f32),
        cost_estimate=pl.CostEstimate(flops=10**9, transcendentals=0, bytes_accessed=2**21),
        compiler_params=limit(4),
        name="suffix",
    )(*(x.reshape(1, slots) for x in (slot_sequence, suffix_lengths)), mine, other, keys, values)
    found_there = across(found)

    part = pl.pallas_call(
        prefix_kernel,
        in_specs=[vmem] * 5,
        out_specs=vmem,
        out_shape=jax.ShapeDtypeStruct((pieces, per_device * local_heads + 8, dim), bf16),
        scratch_shapes=[pltpu.VMEM((2, 2, prefix_keys.shape[0] * kv_local, dim), f32)],
        cost_estimate=pl.CostEstimate(flops=10**9, transcendentals=0, bytes_accessed=2**21),
        compiler_params=limit(6),
        name="prefix",
    )(mine, prefix_keys, prefix_values, *there)
    part = pl.pallas_call(
        merge_kernel,
        in_specs=[vmem] * 3,
        out_specs=vmem,
        out_shape=jax.ShapeDtypeStruct(part.shape, bf16),
        input_output_aliases={0: 0},
        compiler_params=limit(4),
        name="merge",
    )(part, found, found_there)

    got = exchange(part)
    return pl.pallas_call(
        combine_kernel,
        in_specs=[vmem],
        out_specs=vmem,
        out_shape=jax.ShapeDtypeStruct(queries.shape, bf16),
        compiler_params=limit(4),
        name="combine",
    )(got)


def solution(mesh):
    kv, batch = (mesh.shape[a] for a in ("kv", "batch"))
    fine = Mesh(mesh.devices.reshape(kv, batch // 2, 2), ("kv", "m", "core"))
    rows, positions = ("kv", "m", "core"), ("m", "core")
    return jax.shard_map(
        shards,
        mesh=fine,
        in_specs=(
            P(rows, None, None),
            P(positions, "kv", None),
            P(positions, "kv", None),
            P(positions, None, "kv", None),
            P(positions, None, "kv", None),
            P(positions),
            P(positions),
        ),
        out_specs=P(rows, None, None),
        check_vma=False,
    )
```
